32 devices in a mesh: sub: 16 (over z, y, core), tm: 2 (over x).
Axes of the slice: x: 2, y: 2, z: 4, core: 2. Of those that a mesh axis runs over, the one named last changes fastest.
Arguments:
- voltages: bfloat16 [192, 2, 96, 2048], P('sub', None, None, 'tm'), may hold values from -6 to 6
- pointing_table: bfloat16 [192, 2, 320, 96], P('sub'), may hold values from -0.4375 to 0.4375
- beam_pointing: int32 [256], replicated, may hold values from 0 to 319
- subband_order: int32 [192], replicated, may hold values from 0 to 191, each once
- live_subbands: int32 [1], replicated, may hold values from 152 to 192
- filter_taps: float32 [16, 16], replicated, may hold values from -0.36 to 0.36
Outputs:
- synthesised: bfloat16 [256, 12, 2, 32768], P('sub', None, None, 'tm')
The draws below stay inside these ranges and needn't reach their ends.
Inputs may be any that keep to these rules, and one draw needn't show every extreme that they name: `subband_order`: each slot is named by exactly one frequency.
All inputs are finite; a program needn't handle non-finite values.
Results may differ from the reference program's by a relative error of at most 0.0052.
Values may be sent and summed in bfloat16 or wider, within the bound.
No kernel may reach another device: no remote copies, remote signals or barrier semaphores. Data moves between devices by JAX's collectives and lax.ppermute only.
A program may use at most 192 MiB of HBM per device.

```python
import math
import jax
import jax.numpy as jnp
from jax import lax

INPUTS = 96
BEAMS = 256
POINTINGS = 320
CHAN = 16
TAPS = 16
SUBBANDS = 192
TIME = 2048


def draw_live_subbands(key, part):
    span = 2 * CHAN + CHAN // 2
    raw = jax.random.randint(jax.random.fold_in(key, 7919), (1,), -span, span + 1, dtype=jnp.int32)
    missing = jnp.maximum(raw, 0)
    return (SUBBANDS - missing).astype(jnp.int32)


def place_ends(drawn, rng, smallest, top_value):
    longest = drawn.shape.index(max(drawn.shape))
    spots = []
    for shift in (0, 1):
        where = [jax.random.randint(jax.random.fold_in(rng, axis), (), 0, length) for axis, length in enumerate(drawn.shape)]
        where[longest] = (where[longest] + shift) % drawn.shape[longest]
        spots.append(tuple(where))
    return drawn.at[spots[0]].set(smallest).at[spots[1]].set(top_value)


def levels(key, shape, cuts, least, top_value):
    def one(axis_at, blocks):
        steps = jax.random.uniform(jax.random.fold_in(jax.random.fold_in(key, 6), axis_at), (blocks,), jnp.float32, least / len(cuts), top_value / len(cuts))
        return jnp.repeat(jnp.exp(steps), shape[axis_at] // blocks).reshape((-1,) + (1,) * (len(shape) - axis_at - 1))

    loudness = one(*cuts[0])
    for cut in cuts[1:]:
        loudness = loudness * one(*cut)
    return loudness


def gaussian(own_key, dims, spread, bound, pieces=(), held_as=jnp.bfloat16):
    array = spread * jax.random.normal(own_key, dims, jnp.float32)
    if pieces:
        array = array * levels(own_key, dims, pieces, -0.22, 0.18)
    return jnp.clip(array, -bound, bound).astype(held_as)


def setup_inputs(seed: int = 0) -> dict:
    key_of = jax.random.split(jax.random.key(seed), 7)
    return {
        "voltages": gaussian(key_of[0], (SUBBANDS, 2, INPUTS, TIME), 1.0, 6.0, ((0, 16), (3, 2))),
        "pointing_table": gaussian(key_of[1], (SUBBANDS, 2, POINTINGS, INPUTS), (2 * INPUTS) ** -0.5, 0.4375, ((0, 16),)),
        "beam_pointing": place_ends(jax.random.randint(key_of[2], (BEAMS,), 0, POINTINGS), jax.random.fold_in(key_of[2], 1), 0, POINTINGS - 1).astype(jnp.int32),
        "subband_order": jax.random.permutation(key_of[3], SUBBANDS).astype(jnp.int32),
        "live_subbands": draw_live_subbands(jax.random.fold_in(key_of[6], 71), 0),
        "filter_taps": gaussian(key_of[5], (TAPS, CHAN), 0.06, 0.36, (), jnp.float32),
    }


def inverse_table(channel_count):
    channel_index = jnp.arange(channel_count, dtype=jnp.int32)
    phase = (jnp.outer(channel_index, channel_index) % channel_count).astype(jnp.float32) * (2.0 * math.pi / channel_count)
    cosine = jnp.cos(phase).astype(jnp.bfloat16)
    sine_table = jnp.sin(phase).astype(jnp.bfloat16)
    upper_rows = jnp.stack([cosine, -sine_table], axis=1)
    lower_rows = jnp.stack([sine_table, cosine], axis=1)
    return jnp.stack([upper_rows, lower_rows], axis=0)


def reference(voltages, pointing_table, beam_pointing, subband_order, live_subbands, filter_taps):
    highest = lax.Precision.HIGHEST

    def form_subband(subband_pair):
        table_rows, signal = subband_pair
        chosen = jnp.take(table_rows, beam_pointing, axis=1).astype(jnp.float32)
        signal = signal.astype(jnp.float32)
        real_part = jnp.dot(chosen[0], signal[0], precision=highest) - jnp.dot(chosen[1], signal[1], precision=highest)
        imag_part = jnp.dot(chosen[1], signal[0], precision=highest) + jnp.dot(chosen[0], signal[1], precision=highest)
        return jnp.stack([real_part, imag_part], axis=1).astype(jnp.bfloat16)

    formed = lax.map(form_subband, (pointing_table, voltages))
    inverse_rows = inverse_table(CHAN).astype(jnp.float32)
    live_mask = jnp.arange(SUBBANDS, dtype=jnp.int32) < live_subbands[0]
    length = formed.shape[3]

    def synth_beam(beam_index):
        beam_rows = lax.dynamic_index_in_dim(formed, beam_index, 1, keepdims=False)
        spectrum = jnp.take(beam_rows, subband_order, axis=0)
        spectrum = jnp.where(live_mask[:, None, None], spectrum, jnp.zeros_like(spectrum))
        grouped = spectrum.astype(jnp.float32).reshape(SUBBANDS // CHAN, CHAN, 2, length)
        channels = jnp.einsum('qkpc,gcpt->gqkt', inverse_rows, grouped, precision=highest)
        extended = jnp.pad(channels, ((0, 0), (0, 0), (0, 0), (TAPS - 1, 0)))
        running = jnp.zeros_like(channels)
        for tap_index in range(TAPS):
            offset = TAPS - 1 - tap_index
            running = running + filter_taps[tap_index][:, None] * extended[..., offset:offset + length]
        return jnp.swapaxes(running, 2, 3).reshape(SUBBANDS // CHAN, 2, length * CHAN).astype(jnp.bfloat16)

    return lax.map(synth_beam, jnp.arange(BEAMS, dtype=jnp.int32))
```

```python
import functools
import math

import jax
import jax.numpy as jnp
from jax import lax
from jax.experimental import pallas as pl
from jax.experimental.pallas import tpu as pltpu
from jax.sharding import PartitionSpec as P

LANES = 128
CHUNKS = 4


def inverse_table(channel_count):
    channel_index = jnp.arange(channel_count, dtype=jnp.int32)
    phase = (jnp.outer(channel_index, channel_index) % channel_count).astype(jnp.float32) * (
        2.0 * math.pi / channel_count
    )
    cosine = jnp.cos(phase).astype(jnp.bfloat16)
    sine = jnp.sin(phase).astype(jnp.bfloat16)
    upper = jnp.stack([cosine, -sine], axis=0)
    lower = jnp.stack([sine, cosine], axis=0)
    return jnp.stack([upper, lower], axis=0).astype(jnp.float32)


def coefficients(filter_taps, step, shifts):
    taps, channels = filter_taps.shape
    table = inverse_table(channels)
    v = jnp.arange(step)[None, None, :]
    u = jnp.arange(step)[None, :, None]
    s = jnp.arange(shifts)[:, None, None]
    tap = v - u + step * s
    one_hot = (tap[..., None] == jnp.arange(taps)).astype(jnp.float32)
    chosen = jnp.einsum("suvj,jk->suvk", one_hot, filter_taps, precision=lax.Precision.HIGHEST)
    return jnp.einsum(
        "suvk,pqkc->cquspvk", chosen, table, precision=lax.Precision.HIGHEST
    ).reshape(channels * 2 * step, shifts * 2 * step * channels)


def form_kernel(step, table_ref, pick_ref, order_ref, volt_ref, *out_refs):
    pick = pick_ref[...]
    real = jnp.dot(pick, table_ref[0, 0], preferred_element_type=jnp.float32)
    imag = jnp.dot(pick, table_ref[0, 1], preferred_element_type=jnp.float32)
    rows = jnp.concatenate([real, -imag], axis=1).astype(jnp.bfloat16)
    cols = jnp.concatenate([imag, real], axis=1).astype(jnp.bfloat16)
    signal = jnp.dot(volt_ref[0], order_ref[...], preferred_element_type=jnp.float32)
    signal = signal.astype(jnp.bfloat16)
    part = pick.shape[0] // len(out_refs)
    for index, out_ref in enumerate(out_refs):
        mine = slice(index * part, (index + 1) * part)
        up = jnp.dot(rows[mine], signal, preferred_element_type=jnp.float32)
        low = jnp.dot(cols[mine], signal, preferred_element_type=jnp.float32)
        up = up.reshape(part, step, up.shape[1] // step)
        low = low.reshape(part, step, low.shape[1] // step)
        out_ref[0] = jnp.concatenate([up, low], axis=1).astype(jnp.bfloat16)


def synth_kernel(channels, step, shifts, order_ref, live_ref, *refs):
    slots = refs[:channels]
    coef_ref, halo_ref, out_ref = refs[channels:]
    group = pl.program_id(0)
    beams = slots[0].shape[1]
    length = slots[0].shape[3]
    width = 2 * LANES
    stacked = []
    for b in range(beams):
        pieces = []
        for c in range(channels):
            block = slots[c][0, b]
            alive = group * channels + c < live_ref[0]
            pieces.append(jnp.where(alive, block, jnp.zeros_like(block)))
        stacked.append(jnp.concatenate(pieces, axis=0).T)
    lhs = jnp.concatenate(stacked, axis=0)
    sums = jnp.dot(lhs, coef_ref[...], preferred_element_type=jnp.float32)
    row = lax.broadcasted_iota(jnp.int32, (length, width), 0)
    for b in range(beams):
        own = sums[b * length : (b + 1) * length]
        total = own[:, :width]
        for s in range(1, shifts):
            moved = pltpu.roll(own[:, s * width : (s + 1) * width], s, 0)
            total = total + jnp.where(row >= s, moved, 0.0)
        head = total[:8] + halo_ref[0, b]
        total = jnp.concatenate([head, total[8:]], axis=0)
        out_ref[b, 0] = total.reshape(2 * length, LANES).astype(jnp.bfloat16)


def on_device(voltages, pointing_table, beam_pointing, subband_order, live_subbands, filter_taps):
    local = voltages.shape[0]
    inputs = voltages.shape[2]
    time = voltages.shape[3]
    pointings = pointing_table.shape[2]
    beam_count = beam_pointing.shape[0]
    taps, channels = filter_taps.shape
    slot_count = subband_order.shape[0]
    groups = slot_count // channels
    peers = lax.axis_size("sub")
    beam_part = beam_count // peers
    chunks = CHUNKS if beam_part % CHUNKS == 0 else 1
    size = beam_part // chunks
    step = LANES // channels
    blocks = time // step
    shifts = 1 + -(-(taps - 1) // step)
    rim = step * (shifts - 1)
    rows = 2 * step

    signal = voltages.reshape(local, 2 * inputs, time)
    span = lax.axis_size("tm")
    route = [(i - 1, i) for i in range(1, span)]
    edge = lax.ppermute(signal[:, :, time - rim :], "tm", route)

    pointing = beam_pointing.reshape(peers, chunks, size).transpose(1, 0, 2).reshape(-1)
    pick = (pointing[:, None] == jnp.arange(pointings)[None, :]).astype(jnp.bfloat16)
    source = jnp.arange(time, dtype=jnp.int32)
    order = (
        source[:, None] == ((source % blocks) * step + source // blocks)[None, :]
    ).astype(jnp.bfloat16)

    part = beam_count // chunks
    formed = pl.pallas_call(
        functools.partial(form_kernel, step),
        grid=(local,),
        in_specs=[
            pl.BlockSpec((1, 2, pointings, inputs), lambda s: (s, 0, 0, 0)),
            pl.BlockSpec((beam_count, pointings), lambda s: (0, 0)),
            pl.BlockSpec((time, time), lambda s: (0, 0)),
            pl.BlockSpec((1, 2 * inputs, time), lambda s: (s, 0, 0)),
        ],
        out_specs=[pl.BlockSpec((1, part, rows, blocks), lambda s: (s, 0, 0, 0))] * chunks,
        out_shape=[jax.ShapeDtypeStruct((local, part, rows, blocks), jnp.bfloat16)] * chunks,
        compiler_params=pltpu.CompilerParams(dimension_semantics=("arbitrary",)),
        name="form",
    )(pointing_table, pick, order, signal)

    arrived = [
        lax.all_to_all(
            f.reshape(local, peers, size, rows, blocks), "sub", split_axis=1, concat_axis=0, tiled=True
        ).reshape(slot_count, size, rows, blocks)
        for f in formed
    ]

    chosen = jnp.take(pointing_table, beam_pointing, axis=2)
    weight = jnp.concatenate(
        [
            jnp.concatenate([chosen[:, 0], -chosen[:, 1]], axis=2),
            jnp.concatenate([chosen[:, 1], chosen[:, 0]], axis=2),
        ],
        axis=1,
    )
    edge_formed = jnp.einsum(
        "sqi,sit->sqt", weight, edge, preferred_element_type=jnp.float32
    ).astype(jnp.bfloat16)
    edge_formed = edge_formed.reshape(local, 2, peers, beam_part * rim).transpose(0, 2, 1, 3)
    edge_rows = lax.all_to_all(edge_formed, "sub", split_axis=1, concat_axis=0, tiled=True)
    edge_rows = jnp.take(edge_rows[:, 0], subband_order, axis=0)
    live_mask = jnp.arange(slot_count, dtype=jnp.int32) < live_subbands[0]
    edge_rows = jnp.where(live_mask[:, None, None], edge_rows, jnp.zeros_like(edge_rows))
    edge_rows = edge_rows.reshape(groups, channels, 2, beam_part, shifts - 1, step)

    wide = coefficients(filter_taps, step, shifts)
    coef = wide.astype(jnp.bfloat16)
    split = coef.reshape(channels, 2, step, shifts, 2 * LANES)
    parts = []
    for r in range(8):
        terms = jnp.zeros((groups, beam_part, 2 * LANES), jnp.float32)
        for s in range(r + 1, shifts):
            terms = terms + jnp.einsum(
                "gcqbu,cqun->gbn",
                edge_rows[:, :, :, :, shifts - 1 + r - s],
                split[:, :, :, s],
                preferred_element_type=jnp.float32,
            )
        parts.append(terms)
    halo = jnp.stack(parts, axis=2)

    results = []
    for index, block in enumerate(arrived):
        def slot_map(c):
            return lambda g, order_ref, live_ref: (order_ref[g * channels + c], 0, 0, 0)

        results.append(
            pl.pallas_call(
                functools.partial(synth_kernel, channels, step, shifts),
                grid_spec=pltpu.PrefetchScalarGridSpec(
                    num_scalar_prefetch=2,
                    grid=(groups,),
                    in_specs=[
                        pl.BlockSpec((1, size, rows, blocks), slot_map(c)) for c in range(channels)
                    ]
                    + [
                        pl.BlockSpec(coef.shape, lambda g, *_: (0, 0)),
                        pl.BlockSpec((1, size, 8, 2 * LANES), lambda g, *_: (g, index, 0, 0)),
                    ],
                    out_specs=pl.BlockSpec((size, 1, 2 * blocks, LANES), lambda g, *_: (0, g, 0, 0)),
                ),
                out_shape=jax.ShapeDtypeStruct((size, groups, 2 * blocks, LANES), jnp.bfloat16),
                compiler_params=pltpu.CompilerParams(dimension_semantics=("arbitrary",)),
                name="synth",
            )(subband_order, live_subbands, *([block] * channels), coef, halo)
        )
    out = jnp.concatenate(results, axis=0)
    out = out.reshape(beam_part, groups, blocks, 2, LANES).transpose(0, 1, 3, 2, 4)
    return out.reshape(beam_part, groups, 2, blocks * LANES)


def solution(mesh):
    in_specs = (P("sub", None, None, "tm"), P("sub", None, None, None), P(), P(), P(), P())
    out_specs = P("sub", None, None, "tm")
    return jax.shard_map(
        on_device, mesh=mesh, in_specs=in_specs, out_specs=out_specs, check_vma=False
    )
```

```python
import functools
import math

import jax
import jax.numpy as jnp
from jax import lax
from jax.experimental import pallas as pl
from jax.experimental.pallas import tpu as pltpu
from jax.sharding import PartitionSpec as P

LANES = 128


def inverse_table(channel_count):
    channel_index = jnp.arange(channel_count, dtype=jnp.int32)
    phase = (jnp.outer(channel_index, channel_index) % channel_count).astype(jnp.float32) * (
        2.0 * math.pi / channel_count
    )
    cosine = jnp.cos(phase).astype(jnp.bfloat16)
    sine = jnp.sin(phase).astype(jnp.bfloat16)
    upper = jnp.stack([cosine, -sine], axis=0)
    lower = jnp.stack([sine, cosine], axis=0)
    return jnp.stack([upper, lower], axis=0).astype(jnp.float32)


def coefficients(filter_taps, step, shifts):
    taps, channels = filter_taps.shape
    table = inverse_table(channels)
    v = jnp.arange(step)[None, None, :]
    u = jnp.arange(step)[None, :, None]
    s = jnp.arange(shifts)[:, None, None]
    tap = v - u + step * s
    one_hot = (tap[..., None] == jnp.arange(taps)).astype(jnp.float32)
    chosen = jnp.einsum("suvj,jk->suvk", one_hot, filter_taps, precision=lax.Precision.HIGHEST)
    return jnp.einsum(
        "suvk,pqkc->cquspvk", chosen, table, precision=lax.Precision.HIGHEST
    ).reshape(channels * 2 * step, shifts * 2 * step * channels)


def picked(pointing_ref, table_ref):
    rows, choices = pointing_ref.shape[0], table_ref.shape[3]
    at = lax.broadcasted_iota(jnp.int32, (rows, choices), 1)
    pick = (at == pointing_ref[...]).astype(jnp.float32).astype(jnp.bfloat16)
    across = (((1,), (1,)), ((), ()))
    real = lax.dot_general(pick, table_ref[0, 0], across, preferred_element_type=jnp.float32)
    imag = lax.dot_general(pick, table_ref[0, 1], across, preferred_element_type=jnp.float32)
    upper = jnp.concatenate([real, -imag], axis=1).astype(jnp.bfloat16)
    lower = jnp.concatenate([imag, real], axis=1).astype(jnp.bfloat16)
    return upper, lower


def form_kernel(step, pointing_ref, table_ref, volt_ref, out_ref, order_ref):
    time = volt_ref.shape[2]
    blocks = time // step

    @pl.when(pl.program_id(0) == 0)
    def _():
        source = lax.broadcasted_iota(jnp.int32, (time, time), 0)
        place = lax.broadcasted_iota(jnp.int32, (time, time), 1)
        wanted = (place % blocks) * step + place // blocks
        order_ref[...] = (source == wanted).astype(jnp.float32).astype(jnp.bfloat16)

    upper, lower = picked(pointing_ref, table_ref)
    signal = jnp.dot(volt_ref[0], order_ref[...], preferred_element_type=jnp.float32)
    signal = signal.astype(jnp.bfloat16)
    peers, _, size = out_ref.shape[:3]
    up = jnp.dot(upper, signal, preferred_element_type=jnp.float32)
    low = jnp.dot(lower, signal, preferred_element_type=jnp.float32)
    up = up.reshape(peers, size, step, blocks)
    low = low.reshape(peers, size, step, blocks)
    out_ref[:, 0] = jnp.concatenate([up, low], axis=2).astype(jnp.bfloat16)


def rim_kernel(pointing_ref, table_ref, edge_ref, after_ref, out_ref):
    del after_ref
    upper, lower = picked(pointing_ref, table_ref)
    up = jnp.dot(upper, edge_ref[0], preferred_element_type=jnp.float32)
    low = jnp.dot(lower, edge_ref[0], preferred_element_type=jnp.float32)
    out_ref[0, 0] = up.astype(jnp.bfloat16)
    out_ref[0, 1] = low.astype(jnp.bfloat16)


def synth_kernel(channels, step, shifts, order_ref, live_ref, *refs):
    slots = refs[:channels]
    coef_ref, halo_ref, out_ref = refs[channels], refs[channels + 1], refs[-1]
    group = pl.program_id(0)
    beams = slots[0].shape[1]
    length = slots[0].shape[3]
    width = 2 * LANES
    stacked = []
    for b in range(beams):
        pieces = []
        for c in range(channels):
            block = slots[c][0, b]
            alive = group * channels + c < live_ref[0]
            pieces.append(jnp.where(alive, block, jnp.zeros_like(block)))
        stacked.append(jnp.concatenate(pieces, axis=0).T)
    lhs = jnp.concatenate(stacked, axis=0)
    sums = jnp.dot(lhs, coef_ref[...], preferred_element_type=jnp.float32)
    row = lax.broadcasted_iota(jnp.int32, (length, width), 0)
    for b in range(beams):
        own = sums[b * length : (b + 1) * length]
        total = own[:, :width]
        for s in range(1, shifts):
            moved = pltpu.roll(own[:, s * width : (s + 1) * width], s, 0)
            total = total + jnp.where(row >= s, moved, 0.0)
        head = total[:8] + halo_ref[0, b]
        total = jnp.concatenate([head, total[8:]], axis=0)
        out_ref[b, 0] = total.reshape(2 * length, LANES).astype(jnp.bfloat16)


def on_device(voltages, pointing_table, beam_pointing, subband_order, live_subbands, filter_taps):
    local = voltages.shape[0]
    inputs = voltages.shape[2]
    time = voltages.shape[3]
    pointings = pointing_table.shape[2]
    beam_count = beam_pointing.shape[0]
    taps, channels = filter_taps.shape
    slot_count = subband_order.shape[0]
    groups = slot_count // channels
    peers = lax.axis_size("sub")
    beam_part = beam_count // peers
    first, last = max(1, beam_part // 8), max(1, beam_part // 4)
    sizes = [first, beam_part - first - last, last]
    if min(sizes) < 1:
        sizes = [beam_part]
    unit = math.gcd(*sizes)
    step = LANES // channels
    blocks = time // step
    shifts = 1 + -(-(taps - 1) // step)
    rim = step * (shifts - 1)
    rows = 2 * step

    signal = voltages.reshape(local, 2 * inputs, time)
    span = lax.axis_size("tm")
    route = [(i - 1, i) for i in range(1, span)]
    edge = lax.ppermute(signal[:, :, time - rim :], "tm", route)

    table = jnp.swapaxes(pointing_table, 2, 3)
    pointing = beam_pointing.reshape(peers, beam_part)
    per_slot = pl.BlockSpec((1, 2, inputs, pointings), lambda s: (s, 0, 0, 0))

    def form(start, size):
        count = peers * size
        return pl.pallas_call(
            functools.partial(form_kernel, step),
            grid=(local,),
            in_specs=[
                pl.BlockSpec((count, 1), lambda s: (0, 0)),
                per_slot,
                pl.BlockSpec((1, 2 * inputs, time), lambda s: (s, 0, 0)),
            ],
            out_specs=pl.BlockSpec((peers, 1, size, rows, blocks), lambda s: (0, s, 0, 0, 0)),
            out_shape=jax.ShapeDtypeStruct((peers, local, size, rows, blocks), jnp.bfloat16),
            scratch_shapes=[pltpu.VMEM((time, time), jnp.bfloat16)],
            compiler_params=pltpu.CompilerParams(dimension_semantics=("arbitrary",)),
            name="form",
        )(pointing[:, start : start + size].reshape(count, 1), table, signal)

    starts = [sum(sizes[:i]) for i in range(len(sizes))]
    formed = [form(start, size) for start, size in zip(starts, sizes)]
    arrived = [
        lax.all_to_all(f, "sub", split_axis=0, concat_axis=0, tiled=True).reshape(
            slot_count, f.shape[2], rows, blocks
        )
        for f in formed
    ]

    edge_formed = pl.pallas_call(
        rim_kernel,
        grid=(local,),
        in_specs=[
            pl.BlockSpec((beam_count, 1), lambda s: (0, 0)),
            per_slot,
            pl.BlockSpec((1, 2 * inputs, rim), lambda s: (s, 0, 0)),
            pl.BlockSpec(memory_space=pl.ANY),
        ],
        out_specs=pl.BlockSpec((1, 2, beam_count, rim), lambda s: (s, 0, 0, 0)),
        out_shape=jax.ShapeDtypeStruct((local, 2, beam_count, rim), jnp.bfloat16),
        compiler_params=pltpu.CompilerParams(dimension_semantics=("arbitrary",)),
        name="rim",
    )(beam_pointing.reshape(beam_count, 1), table, edge, formed[len(formed) // 2])
    edge_formed = edge_formed.reshape(local, 2, peers, beam_part * rim).transpose(0, 2, 1, 3)
    edge_rows = lax.all_to_all(edge_formed, "sub", split_axis=1, concat_axis=0, tiled=True)
    edge_rows = jnp.take(edge_rows[:, 0], subband_order, axis=0)
    live_mask = jnp.arange(slot_count, dtype=jnp.int32) < live_subbands[0]
    edge_rows = jnp.where(live_mask[:, None, None], edge_rows, jnp.zeros_like(edge_rows))
    edge_rows = edge_rows.reshape(groups, channels, 2, beam_part, shifts - 1, step)

    wide = coefficients(filter_taps, step, shifts)
    coef = wide.astype(jnp.bfloat16)
    split = coef.reshape(channels, 2, step, shifts, 2 * LANES)
    parts = []
    for r in range(8):
        terms = jnp.zeros((groups, beam_part, 2 * LANES), jnp.float32)
        for s in range(r + 1, shifts):
            terms = terms + jnp.einsum(
                "gcqbu,cqun->gbn",
                edge_rows[:, :, :, :, shifts - 1 + r - s],
                split[:, :, :, s],
                preferred_element_type=jnp.float32,
            )
        parts.append(terms)
    halo = jnp.stack(parts, axis=2)

    def slot_map(c):
        return lambda g, i, order_ref, live_ref: (order_ref[g * channels + c], i, 0, 0)

    out = None
    for start, size, block in zip(starts, sizes, arrived):
        base = start // unit
        earlier = [] if out is None else [out]
        out = pl.pallas_call(
            functools.partial(synth_kernel, channels, step, shifts),
            grid_spec=pltpu.PrefetchScalarGridSpec(
                num_scalar_prefetch=2,
                grid=(groups, size // unit),
                in_specs=[
                    pl.BlockSpec((1, unit, rows, blocks), slot_map(c)) for c in range(channels)
                ]
                + [
                    pl.BlockSpec(coef.shape, lambda g, i, *_: (0, 0)),
                    pl.BlockSpec(
                        (1, unit, 8, 2 * LANES), lambda g, i, *_, base=base: (g, base + i, 0, 0)
                    ),
                ]
                + [pl.BlockSpec(memory_space=pl.ANY)] * len(earlier),
                out_specs=pl.BlockSpec(
                    (unit, 1, 2 * blocks, LANES), lambda g, i, *_, base=base: (base + i, g, 0, 0)
                ),
            ),
            out_shape=jax.ShapeDtypeStruct((beam_part, groups, 2 * blocks, LANES), jnp.bfloat16),
            input_output_aliases={channels + 4: 0} if earlier else {},
            compiler_params=pltpu.CompilerParams(dimension_semantics=("arbitrary",) * 2),
            name="synth",
        )(subband_order, live_subbands, *([block] * channels), coef, halo, *earlier)
    out = out.reshape(beam_part, groups, blocks, 2, LANES).transpose(0, 1, 3, 2, 4)
    return out.reshape(beam_part, groups, 2, blocks * LANES)


def solution(mesh):
    in_specs = (P("sub", None, None, "tm"), P("sub", None, None, None), P(), P(), P(), P())
    out_specs = P("sub", None, None, "tm")
    return jax.shard_map(
        on_device, mesh=mesh, in_specs=in_specs, out_specs=out_specs, check_vma=False
    )
```
